32 devices in a mesh: seq: 8 (over z, y), head: 4 (over x, core).
Axes of the slice: x: 2, y: 2, z: 4, core: 2. Of those that a mesh axis runs over, the one named last changes fastest.
Arguments:
- q_low: bfloat16 [2048, 1536], P('seq', 'head'), may hold values from -500 to 500
- q_gain: bfloat16 [1536], P('head'), may hold values from 0.099609375 to 1.8984375
- q_up: bfloat16 [1536, 24576], P(None, 'head'), may hold values from -0.15625 to 0.15625
- key_absorb: bfloat16 [128, 128, 512], P('head'), may hold values from -0.5 to 0.5
- value_absorb: bfloat16 [128, 512, 128], P('head'), may hold values from -0.25 to 0.25
- latent_cache: bfloat16 [65536, 576], P('seq'), may hold values from -1300 to 1300
- tile_picks: int32 [16, 16], P('seq'), may hold values from 0 to 511, as said below
Outputs:
- attended: bfloat16 [2048, 16384], P('seq', 'head')
The draws below stay inside these ranges and needn't reach their ends.
Inputs may be any that keep to these rules, and one draw needn't show every extreme that they name: `tile_picks`: the 16 tiles of one query block differ. Of all tiles that the query blocks of one index of seq select together, at most 8 lie in the cache rows of one index of seq, and exactly 8 in those of some index.
All inputs are finite; a program needn't handle non-finite values.
Results may differ from the reference program's by a relative error of at most 0.03.
Values may be sent and summed in bfloat16 or wider, within the bound.
A program may use at most 192 MiB of HBM per device.

```python
import math
import jax
import jax.numpy as jnp
from jax import lax

HEADS = 128
NOPE = 128
ROPE = 64
LATENT = 512
VDIM = 128
QLORA = 1536
TILE = 128
TOPT = 16
QBLK = 128
CACHE_DEV = 8192
Q_DEV = 256
TOKENS = 2048
CONTEXT = 65536
CAP = 8


def draw_q_low(key, part):
    keys = jax.random.split(key, 3)
    row_scale = jnp.exp(jax.random.uniform(keys[0], (TOKENS, 1), jnp.float32, 0.0, math.log(10.0)))
    column_scale = jnp.exp(jax.random.uniform(keys[1], (1, QLORA), jnp.float32, 0.0, math.log(10.0)))
    base = jnp.clip(jax.random.normal(keys[2], (TOKENS, QLORA), jnp.float32), -5.0, 5.0)
    return (base * row_scale * column_scale).astype(jnp.bfloat16)


def draw_latent_cache(key, part):
    keys = jax.random.split(key, 1)
    width = LATENT + ROPE
    base = jnp.clip(jax.random.normal(keys[0], (CONTEXT, width), jnp.float32), -6.0, 6.0)
    return base.astype(jnp.bfloat16)


def draw_tile_picks(key, part):
    devices = TOKENS // Q_DEV
    count = Q_DEV // QBLK * TOPT
    tiles_dev = CACHE_DEV // TILE
    stride = tiles_dev // CAP

    def one_device(device_key):
        keys = jax.random.split(device_key, 5)
        favoured = jax.random.randint(keys[0], (), 0, devices)
        order = jax.random.permutation(keys[1], devices * CAP)
        ranked = jnp.where(order // CAP == favoured, 0, 1).astype(jnp.int32)
        chosen = order[jnp.argsort(ranked, stable=True)][:count]
        owner = chosen // CAP
        occurrence = chosen % CAP
        offset = jax.random.randint(keys[2], (devices,), 0, tiles_dev)
        inside = jax.random.randint(keys[3], (count,), 0, stride)
        local = (offset[owner] + occurrence * stride + inside) % tiles_dev
        tiles = owner * tiles_dev + local
        tiles = tiles[jax.random.permutation(keys[4], count)]
        return tiles.reshape(Q_DEV // QBLK, TOPT).astype(jnp.int32)
    return jax.vmap(one_device)(jax.random.split(key, devices)).reshape(TOKENS // QBLK, TOPT)


def block_levels(rng, extent, shards, smallest, largest):
    loudness = 1.0
    for axis_at, parts in shards:
        draws = jax.random.uniform(jax.random.fold_in(jax.random.fold_in(rng, 6), axis_at), (parts,), jnp.float32, smallest / len(shards), largest / len(shards))
        loudness = loudness * jnp.repeat(jnp.exp(draws), extent[axis_at] // parts).reshape((-1,) + (1,) * (len(extent) - 1 - axis_at))
    return loudness


def bell_draw(own_key, dims, deviation, limit, cuts=(), kind=jnp.bfloat16):
    drawn = deviation * jax.random.normal(own_key, dims, jnp.float32)
    if cuts:
        drawn = drawn * block_levels(own_key, dims, cuts, -0.22, 0.18)
    return jnp.clip(drawn, -limit, limit).astype(kind)


def setup_inputs(seed: int = 0) -> dict:
    splits = jax.random.split(jax.random.key(seed), 8)
    return {
        "q_low": draw_q_low(jax.random.fold_in(splits[7], 71), 0),
        "q_gain": jnp.clip(1.0 + 0.18 * jax.random.normal(splits[1], (QLORA,), jnp.float32), 0.099609375, 1.8984375).astype(jnp.bfloat16),
        "q_up": bell_draw(splits[2], (QLORA, HEADS * (NOPE + ROPE)), QLORA ** -0.5, 0.15625, ((1, 4),)),
        "key_absorb": bell_draw(splits[3], (HEADS, NOPE, LATENT), NOPE ** -0.5, 0.5, ((0, 4),)),
        "value_absorb": bell_draw(splits[4], (HEADS, LATENT, VDIM), LATENT ** -0.5, 0.25, ((0, 4),)),
        "latent_cache": draw_latent_cache(jax.random.fold_in(splits[7], 71), 0),
        "tile_picks": draw_tile_picks(jax.random.fold_in(splits[7], 71), 0),
    }


def rms_normed(q_low, q_gain):
    values = q_low.astype(jnp.float32)
    power = lax.optimization_barrier(jnp.mean(values * values, axis=-1, keepdims=True))
    return (values * lax.rsqrt(power + 1e-06) * q_gain.astype(jnp.float32)).astype(jnp.bfloat16)

def rotate(rope, positions):
    half = rope.shape[-1] // 2
    freq = jnp.power(jnp.float32(10000.0), -(2.0 * jnp.arange(half, dtype=jnp.float32)) / rope.shape[-1])
    angle = positions.astype(jnp.float32)[:, None] * freq[None, :]
    cosine = jnp.cos(angle)[:, None, :]
    sine = jnp.sin(angle)[:, None, :]
    first = rope[..., :half].astype(jnp.float32)
    second = rope[..., half:].astype(jnp.float32)
    return jnp.concatenate([first * cosine - second * sine, first * sine + second * cosine], axis=-1).astype(jnp.bfloat16)

def reference(q_low, q_gain, q_up, key_absorb, value_absorb, latent_cache, tile_picks):
    tokens = q_low.shape[0]
    width = latent_cache.shape[1]
    normed = rms_normed(q_low, q_gain)
    query = jnp.dot(normed, q_up, preferred_element_type=jnp.float32).astype(jnp.bfloat16)
    query = query.reshape(tokens, HEADS, NOPE + ROPE)
    positions = CONTEXT + jnp.arange(tokens, dtype=jnp.int32)
    rotated = rotate(query[..., NOPE:], positions)
    latent_q = jnp.einsum('thn,hnl->thl', query[..., :NOPE].astype(jnp.float32), key_absorb.astype(jnp.float32)).astype(jnp.bfloat16)
    full_q = jnp.concatenate([latent_q, rotated], axis=-1).reshape(tokens // QBLK, QBLK * HEADS, width)
    tiles = latent_cache.reshape(CONTEXT // TILE, TILE, width)
    scale = float(NOPE + ROPE) ** (-0.5)

    def one_block(operands):
        block_q, picks = operands
        keys = jnp.take(tiles, picks.astype(jnp.int32), axis=0).reshape(TOPT * TILE, width)
        scores = jnp.dot(block_q, keys.T, preferred_element_type=jnp.float32) * scale
        weights = jax.nn.softmax(scores, axis=-1).astype(jnp.bfloat16)
        return jnp.dot(weights, keys[:, :LATENT], preferred_element_type=jnp.float32).astype(jnp.bfloat16)
    mixed = lax.map(one_block, (full_q, tile_picks)).reshape(tokens, HEADS, LATENT)
    attended = jnp.einsum('thl,hlv->thv', mixed.astype(jnp.float32), value_absorb.astype(jnp.float32))
    return attended.astype(jnp.bfloat16).reshape(tokens, HEADS * VDIM)
```

```python
import jax
import jax.numpy as jnp
from jax import lax
from jax.experimental import pallas as pl
from jax.experimental.pallas import tpu as pltpu
from jax.sharding import PartitionSpec as P

NOPE = 128
ROPE = 64
LATENT = 512
VDIM = 128
TILE = 128
TOPT = 16
QBLK = 128
LANES = 128
LOG2E = 1.4426950408889634


def rms_normed(q_low, q_gain):
    values = q_low.astype(jnp.float32)
    power = jnp.mean(values * values, axis=-1, keepdims=True)
    return (values * lax.rsqrt(power + 1e-06) * q_gain.astype(jnp.float32)).astype(jnp.bfloat16)


def rotary_tables(positions):
    half = ROPE // 2
    freq = jnp.power(
        jnp.float32(10000.0), -(2.0 * jnp.arange(half, dtype=jnp.float32)) / ROPE
    )
    angle = positions.astype(jnp.float32)[:, None] * freq[None, :]
    cosine, sine = jnp.cos(angle), jnp.sin(angle)
    return (
        jnp.concatenate([cosine, cosine], axis=-1),
        jnp.concatenate([-sine, sine], axis=-1),
    )


def absorb_kernel(query_ref, absorb_ref, cos_ref, sin_ref, out_ref):
    heads = absorb_ref.shape[0]
    rows = query_ref.shape[0]
    half = ROPE // 2
    cosine, sine = cos_ref[...], sin_ref[...]
    for head in range(heads):
        start = head * (NOPE + ROPE)
        nope = query_ref[:, start : start + NOPE]
        rope = query_ref[:, start + NOPE : start + NOPE + ROPE].astype(jnp.float32)
        swapped = jnp.concatenate([rope[:, half:], rope[:, :half]], axis=-1)
        rotated = rope * cosine + swapped * sine
        out_ref[head, :, :LATENT] = jnp.dot(
            nope, absorb_ref[head], preferred_element_type=jnp.float32
        ).astype(jnp.bfloat16)
        out_ref[head, :, LATENT:] = jnp.concatenate(
            [rotated, jnp.zeros((rows, LANES - ROPE), jnp.float32)], axis=-1
        ).astype(jnp.bfloat16)


def absorbed_query(query, key_absorb, cosine, sine):
    rows = query.shape[0]
    group = key_absorb.shape[0]
    step = min(8, group)
    width = LATENT + LANES
    return pl.pallas_call(
        absorb_kernel,
        grid=(group // step,),
        in_specs=[
            pl.BlockSpec((rows, step * (NOPE + ROPE)), lambda i: (0, i)),
            pl.BlockSpec((step, NOPE, LATENT), lambda i: (i, 0, 0)),
            pl.BlockSpec((rows, ROPE), lambda i: (0, 0)),
            pl.BlockSpec((rows, ROPE), lambda i: (0, 0)),
        ],
        out_specs=pl.BlockSpec((step, rows, width), lambda i: (i, 0, 0)),
        out_shape=jax.ShapeDtypeStruct((group, rows, width), jnp.bfloat16),
        cost_estimate=pl.CostEstimate(
            flops=2 * rows * group * NOPE * LATENT,
            bytes_accessed=2 * (query.size + key_absorb.size + group * rows * width),
            transcendentals=0,
        ),
        name="absorb",
    )(query, key_absorb, cosine, sine)


def attend_kernel(query_ref, keys_ref, absorb_ref, out_ref, turned, values):
    heads = absorb_ref.shape[0]
    tiles, width = keys_ref.shape[1:3]

    @pl.when(pl.program_id(1) == 0)
    def _():
        turned[width:, :] = jnp.zeros((turned.shape[0] - width, turned.shape[1]), turned.dtype)
        for tile in range(tiles):
            span = slice(tile * TILE, (tile + 1) * TILE)
            turned[:width, span] = keys_ref[0, tile]
            values[span, :] = keys_ref[0, tile, :LATENT, :].T

    scale = float(NOPE + ROPE) ** (-0.5) * LOG2E
    pair = 2
    scores = []
    for at in range(0, heads, pair):
        block = query_ref[at : at + pair].reshape(pair * QBLK, query_ref.shape[2])
        scores.append(
            jnp.dot(block, turned[...], preferred_element_type=jnp.float32)
        )
    for at in range(0, heads, pair):
        score = scores[at // pair]
        top = jnp.max(score, axis=-1, keepdims=True)
        weights = jnp.exp2((score - top) * scale)
        total = jnp.sum(weights, axis=-1, keepdims=True)
        mixed = jnp.dot(
            weights.astype(jnp.bfloat16),
            values[...],
            preferred_element_type=jnp.float32,
        )
        mixed = (mixed / total).astype(jnp.bfloat16)
        for head in range(pair):
            out_ref[:, (at + head) * VDIM : (at + head + 1) * VDIM] = jnp.dot(
                mixed[head * QBLK : (head + 1) * QBLK],
                absorb_ref[at + head],
                preferred_element_type=jnp.float32,
            ).astype(jnp.bfloat16)


def attend(full_q, keys, value_absorb):
    group, rows, padded = full_q.shape
    blocks, tiles, width = keys.shape[:3]
    count = tiles * TILE
    step = min(4, group)
    return pl.pallas_call(
        attend_kernel,
        grid=(blocks, group // step),
        in_specs=[
            pl.BlockSpec((step, QBLK, padded), lambda b, g: (g, b, 0)),
            pl.BlockSpec((1, tiles, width, TILE), lambda b, g: (b, 0, 0, 0)),
            pl.BlockSpec((step, LATENT, VDIM), lambda b, g: (g, 0, 0)),
        ],
        out_specs=pl.BlockSpec((QBLK, step * VDIM), lambda b, g: (b, g)),
        out_shape=jax.ShapeDtypeStruct((rows, group * VDIM), jnp.bfloat16),
        scratch_shapes=[
            pltpu.VMEM((padded, count), jnp.bfloat16),
            pltpu.VMEM((count, LATENT), jnp.bfloat16),
        ],
        compiler_params=pltpu.CompilerParams(
            dimension_semantics=("arbitrary", "arbitrary"), vmem_limit_bytes=60 * 1024 * 1024
        ),
        cost_estimate=pl.CostEstimate(
            flops=2 * rows * group * count * (padded + LATENT),
            bytes_accessed=2 * (full_q.size + keys.size + value_absorb.size * blocks),
            transcendentals=rows * group * count,
        ),
        name="attend",
    )(full_q, keys, value_absorb)


def owner_rank(picks, tiles_dev):
    owner = picks // tiles_dev
    order = jnp.arange(picks.shape[0], dtype=jnp.int32)
    same = picks[:, None] == picks[None, :]
    first = jnp.min(jnp.where(same, order[None, :], picks.shape[0]), axis=1)
    fresh = first == order
    before = (owner[:, None] == owner[None, :]) & fresh[None, :] & (order[None, :] < first[:, None])
    return (owner, jnp.sum(before.astype(jnp.int32), axis=1), fresh)


def place_table(place, local, length):
    hit = place[:, None] == jnp.arange(length, dtype=jnp.int32)[None, :]
    return jnp.sum(jnp.where(hit, local[:, None], 0), axis=0)


def body(q_low, q_gain, q_up, key_absorb, value_absorb, latent_cache, tile_picks):
    whole_low, whole_gain = (
        lax.all_gather(q_low, "head", axis=1, tiled=True),
        lax.all_gather(q_gain, "head", axis=0, tiled=True),
    )
    rows = whole_low.shape[0]
    width = latent_cache.shape[1]
    seq_count = lax.axis_size("seq")
    tiles_dev = latent_cache.shape[0] // TILE
    picks = tile_picks.reshape(-1)
    count = picks.shape[0]
    cap = max(2, 2 * count // seq_count)
    owner, rank, fresh = owner_rank(picks, tiles_dev)
    share = width // lax.axis_size("head")
    columns = lax.dynamic_slice_in_dim(latent_cache, lax.axis_index("head") * share, share, 1)
    cache_tiles = columns.T.reshape(share, tiles_dev, TILE).transpose(1, 0, 2)
    requests = place_table(
        owner * cap + rank, jnp.where(fresh, picks % tiles_dev, 0), seq_count * cap
    ).reshape(
        seq_count, cap
    )
    serve_requests = lax.all_to_all(requests, "seq", split_axis=0, concat_axis=0, tiled=True)
    found = jnp.take(cache_tiles, serve_requests, axis=0, mode="clip")
    fetched = lax.all_to_all(found, "seq", split_axis=0, concat_axis=0, tiled=True)
    flat = fetched.reshape(seq_count * cap, share, TILE)
    keys = jnp.take(flat, owner * cap + rank, axis=0, mode="clip")
    normed = rms_normed(whole_low, whole_gain)
    query = jnp.dot(normed, q_up, preferred_element_type=jnp.float32).astype(jnp.bfloat16)
    keys, query = lax.optimization_barrier((keys, query))
    keys = lax.all_gather(keys, "head", axis=1, tiled=True)
    keys = keys.reshape(count // TOPT, TOPT, width, TILE)
    context = latent_cache.shape[0] * seq_count
    positions = context + lax.axis_index("seq") * rows + jnp.arange(rows, dtype=jnp.int32)
    full_q = absorbed_query(query, key_absorb, *rotary_tables(positions))
    return attend(full_q, keys, value_absorb)


def solution(mesh):
    in_specs = (
        P("seq", "head"),
        P("head"),
        P(None, "head"),
        P("head", None, None),
        P("head", None, None),
        P("seq", None),
        P("seq", None),
    )
    out_specs = P("seq", "head")
    return jax.shard_map(body, mesh=mesh, in_specs=in_specs, out_specs=out_specs, check_vma=False)
```
